512 devices in a mesh: row: 32 (over y_hi, x, core), col: 16 (over y_lo, z).
Axes of the slice: x: 4, y: 8 (y_hi: 4, y_lo: 2; y = y_hi * 2 + y_lo), z: 8, core: 2. Of those that a mesh axis runs over, the one named last changes fastest.
Arguments:
- amplitudes: bfloat16 [1024, 32768], P('row', 'col'), may hold values from -6 to 6
- integrals: bfloat16 [32768, 32768], P('col', 'row'), may hold values from -0.0390625 to 0.0390625
- tile_mask: int32 [256, 256], P('col', 'row'), may hold values 0 or 1
- driving: bfloat16 [1024, 32768], P('col', 'row'), may hold values from -6 to 6
- occupied_energy: float32 [1024], P('col'), may hold values from -1.5 to -0.5
- virtual_energy: float32 [32768], P('row'), may hold values from 0.5 to 2.5
Outputs:
- update: float32 [1024, 32768], P('col', 'row')
The draws below stay inside these ranges and needn't reach their ends.
All inputs are finite; a program needn't handle non-finite values. No bound on the sum of `tile_mask` on one device may be relied on, other than what follows from the above.
Results may differ from the reference program's by a relative error of at most 0.0003.
Values may be sent and summed in bfloat16 or wider, within the bound.
A program may use at most 64 MiB of HBM per device.

```python
import math
import jax
import jax.numpy as jnp
from jax import lax

VP = 32768
TILE = 128
ROWS = 1024
NT = 256


def with_ends(drawn, rng, smallest, top_value):
    longest = drawn.shape.index(max(drawn.shape))
    spots = []
    for shift in (0, 1):
        where = [jax.random.randint(jax.random.fold_in(rng, axis), (), 0, length) for axis, length in enumerate(drawn.shape)]
        where[longest] = (where[longest] + shift) % drawn.shape[longest]
        spots.append(tuple(where))
    return drawn.at[spots[0]].set(smallest).at[spots[1]].set(top_value)


def steps_of(rng, extent, split, smallest, top_value):
    level, own = 1.0, jax.random.fold_in(rng, 6)
    for axis_at, shards_of in split:
        steps = jnp.exp(jax.random.uniform(jax.random.fold_in(own, axis_at), (shards_of,), jnp.float32, smallest / len(split), top_value / len(split)))
        level = level * jnp.repeat(steps, extent[axis_at] // shards_of).reshape([-1 if axis == axis_at else 1 for axis in range(len(extent))])
    return level


def scatter_about(own_key, shape, scale, reach, pieces=(), held_as=jnp.bfloat16):
    drawn = scale * jax.random.normal(own_key, shape, jnp.float32)
    if pieces:
        drawn = drawn * steps_of(own_key, shape, pieces, -0.22, 0.18)
    return jnp.clip(drawn, -reach, reach).astype(held_as)


def setup_inputs(seed: int = 0) -> dict:
    splits = jax.random.split(jax.random.key(seed), 7)
    amplitudes = scatter_about(splits[0], (ROWS, VP), 1.0, 6.0, ((0, 32), (1, 16)))
    integrals = scatter_about(splits[1], (VP, VP), (3 * VP // 5) ** -0.5, 0.0390625, ((0, 16), (1, 32)))
    tile_mask = with_ends((jax.random.randint(splits[2], (NT, NT), 0, 5) < 3).astype(jnp.int32), jax.random.fold_in(splits[2], 1), 0, 1)
    driving = scatter_about(splits[3], (ROWS, VP), 1.0, 6.0, ((0, 16), (1, 32)))
    occupied_energy = jnp.clip(-1.5 + 1.0 * jax.random.uniform(splits[4], (ROWS,), jnp.float32) ** steps_of(splits[4], (ROWS,), ((0, 16),), -0.2, 0.2), -1.5, -0.5)
    virtual_energy = jnp.clip(jnp.exp(math.log(2.5) - 1.609438 * jax.random.uniform(splits[5], (VP,), jnp.float32) ** steps_of(splits[5], (VP,), ((0, 32),), -0.2, 0.2)), 0.5, 2.5)
    return dict(amplitudes=amplitudes, integrals=integrals, tile_mask=tile_mask, driving=driving, occupied_energy=occupied_energy, virtual_energy=virtual_energy)


def reference(amplitudes, integrals, tile_mask, driving, occupied_energy, virtual_energy):
    width = 16 * TILE
    blocks = VP // width
    mask_vals = tile_mask.astype(jnp.bfloat16)

    def one_block(index):
        start = (index * width).astype(jnp.int32)
        columns = lax.dynamic_slice_in_dim(integrals, start, width, 1)
        tiles = lax.dynamic_slice_in_dim(mask_vals, (index * 16).astype(jnp.int32), 16, 1)
        shaped = columns.reshape(NT, TILE, 16, TILE) * tiles[:, None, :, None]
        masked = shaped.reshape(VP, width)
        return jnp.dot(amplitudes, masked, preferred_element_type=jnp.float32)

    parts = lax.map(one_block, jnp.arange(blocks, dtype=jnp.int32))
    ladder = jnp.transpose(parts, (1, 0, 2)).reshape(ROWS, VP)
    denom = virtual_energy[None, :] - occupied_energy[:, None]
    return (driving.astype(jnp.float32) + ladder) / denom
```

```python
import functools

import jax
import jax.numpy as jnp
from jax import lax
from jax.experimental import pallas as pl
from jax.experimental.pallas import tpu as pltpu
from jax.sharding import PartitionSpec as P

MESH = pl.DeviceIdType.MESH
TOP = 32767.0
TINY = 1e-30

UNITS = (
    (0, 0),
    (1, 0), (-1, 0),
    (2, 0), (0, 1), (0, -1),
    (1, 1), (1, -1), (-1, 1), (-1, -1), (0, 2),
    (2, 1), (2, -1), (1, 2), (-1, 2),
    (2, 2),
)
SLOT = {unit: slot for slot, unit in enumerate(UNITS)}
GROUPS = ((0, 1), (1, 3), (3, 6), (6, 11), (11, 15), (15, 16))
GROUP_AT = (3.5, 6.5, 10.5, 15.5, 19.0, 21.5)
HOP = 4.0
DYS = (0, 1, -1, 2)


def kernel(a_ref, m_hbm, mask_ref, out_ref, held, m_ref, part, q_out, s_out, q_in, s_in, total, yq_out, ys_out, yq_in, ys_in,
           m_sem, own_sem, ag_send, ag_recv, z_send, z_recv, zs_send, zs_recv, y_sem):
    row, col = lax.axis_index("row"), lax.axis_index("col")
    core = lax.rem(row, 2)
    x = lax.rem(row // 2, 4)
    y = row // 8
    z = lax.rem(col, 8)
    y_lo = col // 8
    depth = a_ref.shape[0]
    half = depth // 2
    rows = 2 * depth

    def at_xy(dx, dy):
        return ((lax.rem(y + dy + 4, 4) * 4 + lax.rem(x + dx + 4, 4)) * 2 + core, col)

    def at_z(dz):
        return (row, y_lo * 8 + lax.rem(z + dz + 8, 8))

    sibling = ((y * 4 + x) * 2 + (1 - core), col)
    mate = (row, (1 - y_lo) * 8 + z)
    partners = (at_xy(1, 0), at_xy(-1, 0), at_xy(0, 1), at_xy(0, -1), sibling, at_z(1), at_z(-1), mate)

    chunks = m_sem.shape[0]
    step = m_ref.shape[0] // chunks
    loads = [
        pltpu.make_async_copy(m_hbm.at[pl.ds(i * step, step)], m_ref.at[pl.ds(i * step, step)], m_sem.at[i])
        for i in range(chunks)
    ]
    for load in loads:
        load.start()
    own = pltpu.make_async_copy(a_ref, held.at[pl.ds(core * depth, depth)], own_sem)
    own.start()

    barrier = pltpu.get_barrier_semaphore()
    for partner in partners:
        pl.semaphore_signal(barrier, inc=1, device_id=partner, device_id_type=MESH)
    pl.semaphore_wait(barrier, len(partners))

    kinds = {}

    def piece(unit, part_of):
        start = SLOT[unit] * rows + core * depth
        if part_of is None:
            return held.at[pl.ds(start, depth)]
        return held.at[pl.ds(start + part_of * half, half)]

    def message(kind, source, target_unit, part_of, device):
        index = kinds.setdefault(kind, len(kinds))
        return pltpu.make_async_remote_copy(
            src_ref=source, dst_ref=piece(target_unit, part_of), send_sem=ag_send.at[index], recv_sem=ag_recv.at[index],
            device_id=device, device_id_type=MESH)

    sent = {}

    def send(kind, source, target_unit, part_of, device):
        copy = message(kind, source, target_unit, part_of, device)
        copy.start()
        sent[kind] = copy

    def own_half(h):
        return a_ref.at[pl.ds(h * half, half)]

    def source(unit, h):
        if unit == (0, 0):
            return a_ref if h is None else own_half(h)
        return piece(unit, h)

    def wrap(d):
        return 2 if d == -2 else d

    def got(kind):
        sent[kind].wait_recv()

    def to_sibling(unit, h=None):
        send(("s", unit, h), source(unit, h), unit, h, sibling)

    def x_first(dy, h):
        order = (1, -1) if h == 0 else (-1, 1)
        for dx in order:
            send(("x1", dx, dy, h), source((0, dy), h), (-dx, dy), h, at_xy(dx, 0))

    def x_second(dx, dy):
        h = 0 if dx == 1 else 1
        send(("x2", dx, dy), piece((-dx, dy), h), (2, dy), h, at_xy(dx, 0))

    def y_second(dy):
        h = 0 if dy == 1 else 1
        send(("y2", dy), piece((0, -dy), h), (0, 2), h, at_xy(0, dy))

    def act_y1(dy, h):
        def run():
            got(("y1", dy, h))
            first = 0 if dy == 1 else 1
            if h == first:
                y_second(dy)
            x_first(-dy, h)
            if h != first:
                to_sibling((0, -dy))
        return run

    def act_y2(dy):
        def run():
            got(("y2", dy))
            h = 0 if dy == 1 else 1
            x_first(2, h)
            to_sibling((0, 2), h)
        return run

    def act_x1(dx, dy, h):
        def run():
            got(("x1", dx, dy, h))
            if h == (0 if dx == 1 else 1):
                x_second(dx, dy)
            to_sibling((-dx, dy), h)
        return run

    def act_x2(dx, dy):
        def run():
            got(("x2", dx, dy))
            to_sibling((2, dy), 0 if dx == 1 else 1)
        return run

    for h in (0, 1):
        for dy in (1, -1):
            ph = h if dy == 1 else 1 - h
            send(("y1", dy, ph), own_half(ph), (0, -dy), ph, at_xy(0, dy))
        for dx in (1, -1):
            ph = h if dx == 1 else 1 - h
            send(("x1", dx, 0, ph), own_half(ph), (-dx, 0), ph, at_xy(dx, 0))
        if h == 0:
            to_sibling((0, 0))

    tiles = 128
    for i in range(chunks):
        loads[i].wait()

        @pl.loop(0, step // tiles)
        def _(t, i=i):
            for j in range(m_ref.shape[1] // tiles):
                filled = mask_ref[i * (step // tiles) + t, j].astype(jnp.float32)
                here = (pl.ds(pl.multiple_of(i * step + t * tiles, tiles), tiles), pl.ds(j * tiles, tiles))
                m_ref[here] = m_ref[here] * filled.astype(jnp.bfloat16)

    own.wait()

    wide = 256

    def act_mm(lo, hi):
        def run():
            for slot in range(lo, hi):
                for kind in sibling_kinds[slot]:
                    got(kind)
            span = pl.ds(lo * rows, (hi - lo) * rows)

            @pl.loop(0, m_ref.shape[1] // wide)
            def _(n):
                across = pl.ds(pl.multiple_of(n * wide, wide), wide)
                part[span, across] = jnp.dot(held[span, :], m_ref[:, across], preferred_element_type=jnp.float32)
        return run

    lanes = 256

    def encode(value, q_ref, s_ref, t):
        top = jnp.max(jnp.abs(value), axis=0, keepdims=True)
        top = jnp.maximum(top, TINY)
        q_ref[:, pl.ds(pl.multiple_of(t * lanes, lanes), lanes)] = jnp.round(value * (TOP / top)).astype(jnp.int16)
        s_ref[pl.ds(t, 1), :] = top * (1.0 / TOP)

    def decode(q_ref, s_ref, t):
        return q_ref[:, pl.ds(pl.multiple_of(t * lanes, lanes), lanes)].astype(jnp.float32) * s_ref[pl.ds(t, 1), :]

    def over_lanes(body):
        pl.loop(0, part.shape[1] // lanes)(body)

    def where_is(slot):
        dx, dy = UNITS[slot]
        ux, uy = lax.rem(x + dx + 4, 4), lax.rem(y + dy + 4, 4)
        lo = uy // 2
        d = lax.rem(z - (lax.rem(uy, 2) * 4 + ux) + 8, 8)
        down = (d < 4) | ((d == 4) & (lo == 0))
        p = jnp.where(d <= 4, d, 8 - d)
        first = (p == 4) | ((p == 3) & (down != (lo == 0)))
        return d, p, down, first, lo

    def z_copies(slot, way):
        device = at_z(-1 if way == 0 else 1)
        return (
            pltpu.make_async_remote_copy(
                src_ref=q_out.at[slot], dst_ref=q_in.at[slot, way], send_sem=z_send.at[slot], recv_sem=z_recv.at[slot, way],
                device_id=device, device_id_type=MESH),
            pltpu.make_async_remote_copy(
                src_ref=s_out.at[slot], dst_ref=s_in.at[slot, way], send_sem=zs_send.at[slot], recv_sem=zs_recv.at[slot, way],
                device_id=device, device_id_type=MESH),
        )

    def z_start(slot, down):
        for way in (0, 1):
            @pl.when(down if way == 0 else jnp.logical_not(down))
            def _():
                for copy in z_copies(slot, way):
                    copy.start()

    def own_part(slot, t):
        return part[pl.ds(slot * rows, rows), pl.ds(pl.multiple_of(t * lanes, lanes), lanes)]

    def act_start(slot):
        def run():
            d, p, down, first, lo = where_is(slot)

            @pl.when(first)
            def _():
                over_lanes(lambda t: encode(own_part(slot, t), q_out.at[slot], s_out.at[slot], t))
                z_start(slot, down)
        return run

    def act_hop(slot, at):
        def run():
            d, p, down, first, lo = where_is(slot)
            for way in (0, 1):
                @pl.when((p == at) & jnp.logical_not(first) & (down if way == 0 else jnp.logical_not(down)))
                def _():
                    for copy in z_copies(slot, way):
                        copy.wait_recv()
                    over_lanes(lambda t: encode(
                        own_part(slot, t) + decode(q_in.at[slot, way], s_in.at[slot, way], t),
                        q_out.at[slot], s_out.at[slot], t))
                    for copy in z_copies(slot, way):
                        copy.start()
        return run

    y_copies = (
        pltpu.make_async_remote_copy(src_ref=yq_out, dst_ref=yq_in, send_sem=y_sem.at[0], recv_sem=y_sem.at[1],
                                     device_id=mate, device_id_type=MESH),
        pltpu.make_async_remote_copy(src_ref=ys_out, dst_ref=ys_in, send_sem=y_sem.at[2], recv_sem=y_sem.at[3],
                                     device_id=mate, device_id_type=MESH),
    )

    def act_end(slot):
        def run():
            d, p, down, first, lo = where_is(slot)

            @pl.when(d == 0)
            def _():
                for way in (0, 1):
                    for copy in z_copies(slot, way):
                        copy.wait_recv()

                def summed(t):
                    return (own_part(slot, t) + decode(q_in.at[slot, 0], s_in.at[slot, 0], t)
                            + decode(q_in.at[slot, 1], s_in.at[slot, 1], t))

                @pl.when(lo != y_lo)
                def _():
                    over_lanes(lambda t: encode(summed(t), yq_out, ys_out, t))
                    for copy in y_copies:
                        copy.start()

                @pl.when(lo == y_lo)
                def _():
                    def keep(t):
                        total[:, pl.ds(pl.multiple_of(t * lanes, lanes), lanes)] = summed(t)
                    over_lanes(keep)
        return run

    acts = []
    for dx in (1, -1):
        f = 0 if dx == 1 else 1
        acts.append((3.0, act_x1(dx, 0, f)))
        acts.append((4.5, act_x1(dx, 0, 1 - f)))
        acts.append((6.3, act_x2(dx, 0)))
        for dy in (1, -1):
            acts.append((9.0, act_x1(dx, dy, f)))
            acts.append((12.0, act_x1(dx, dy, 1 - f)))
            acts.append((13.5, act_x2(dx, dy)))
        acts.append((14.8, act_x1(dx, 2, f)))
        acts.append((16.0, act_x1(dx, 2, 1 - f)))
        acts.append((18.5, act_x2(dx, 2)))
    for dy in (1, -1):
        f = 0 if dy == 1 else 1
        acts.append((5.3, act_y1(dy, f)))
        acts.append((8.1, act_y1(dy, 1 - f)))
        acts.append((11.3, act_y2(dy)))
    for (lo, hi), at in zip(GROUPS, GROUP_AT):
        acts.append((at, act_mm(lo, hi)))
        for slot in range(lo, hi):
            acts.append((at + 0.01, act_start(slot)))
            for k in (3, 2, 1):
                acts.append((at + 1.0 + HOP * (4 - k), act_hop(slot, k)))
            acts.append((at + 1.0 + HOP * 4, act_end(slot)))
    acts.sort(key=lambda act: act[0])

    sibling_kinds = []
    for unit in UNITS:
        dx, dy = unit
        whole = dx == 0 and dy != 2
        sibling_kinds.append([("s", unit, None)] if whole else [("s", unit, 0), ("s", unit, 1)])

    for _, run in acts:
        run()

    for copy in y_copies:
        copy.wait_recv()

    def finish(t):
        across = pl.ds(pl.multiple_of(t * lanes, lanes), lanes)
        out_ref[:, across] = total[:, across] + decode(yq_in, ys_in, t)
    over_lanes(finish)

    for copy in sent.values():
        copy.wait_send()
    for slot in range(len(UNITS)):
        d = where_is(slot)[0]

        @pl.when(d != 0)
        def _():
            for copy in z_copies(slot, 0):
                copy.wait_send()
    for copy in y_copies:
        copy.wait_send()


def gathered_product(amplitudes, integrals, tile_mask):
    depth, inner = amplitudes.shape
    width = integrals.shape[1]
    rows = 2 * depth
    n = len(UNITS)
    groups = width // 256
    vmem = pltpu.VMEM
    dma = pltpu.SemaphoreType.DMA
    messages = 64
    return pl.pallas_call(
        kernel,
        out_shape=jax.ShapeDtypeStruct((rows, width), jnp.float32),
        in_specs=[
            pl.BlockSpec(memory_space=pltpu.VMEM),
            pl.BlockSpec(memory_space=pl.ANY),
            pl.BlockSpec(memory_space=pltpu.SMEM),
        ],
        out_specs=pl.BlockSpec(memory_space=pltpu.VMEM),
        scratch_shapes=[
            vmem((n * rows, inner), jnp.bfloat16),
            vmem((inner, width), jnp.bfloat16),
            vmem((n * rows, width), jnp.float32),
            vmem((n, rows, width), jnp.int16),
            vmem((n, groups, 256), jnp.float32),
            vmem((n, 2, rows, width), jnp.int16),
            vmem((n, 2, groups, 256), jnp.float32),
            vmem((rows, width), jnp.float32),
            vmem((rows, width), jnp.int16),
            vmem((groups, 256), jnp.float32),
            vmem((rows, width), jnp.int16),
            vmem((groups, 256), jnp.float32),
            dma((4,)),
            dma,
            dma((messages,)),
            dma((messages,)),
            dma((n,)),
            dma((n, 2)),
            dma((n,)),
            dma((n, 2)),
            dma((4,)),
        ],
        compiler_params=pltpu.CompilerParams(
            collective_id=0, has_side_effects=True, vmem_limit_bytes=48 * 1024 * 1024),
        name="ladder",
    )(amplitudes, integrals, tile_mask)


def shards(amplitudes, integrals, tile_mask, driving, occupied_energy, virtual_energy):
    ladder = gathered_product(amplitudes, integrals, tile_mask)
    denom = virtual_energy[None, :] - occupied_energy[:, None]
    return (driving.astype(jnp.float32) + ladder) / denom


def solution(mesh):
    in_specs = (
        P("row", "col"),
        P("col", "row"),
        P("col", "row"),
        P("col", "row"),
        P("col"),
        P("row"),
    )
    out_specs = P("col", "row")
    return jax.shard_map(shards, mesh=mesh, in_specs=in_specs, out_specs=out_specs, check_vma=False)
```

```python
import functools

import jax
import jax.numpy as jnp
from jax import lax
from jax.experimental import pallas as pl
from jax.experimental.pallas import tpu as pltpu
from jax.sharding import PartitionSpec as P

MESH = pl.DeviceIdType.MESH
TOP = 32767.0
TINY = 1e-30

UNITS = (
    (0, 0),
    (1, 0), (-1, 0),
    (2, 0), (0, 1), (0, -1),
    (1, 1), (1, -1), (-1, 1), (-1, -1), (0, 2),
    (2, 1), (2, -1), (1, 2), (-1, 2),
    (2, 2),
)
SLOT = {unit: slot for slot, unit in enumerate(UNITS)}
GROUPS = ((0, 1), (1, 3), (3, 6), (6, 11), (11, 15), (15, 16))
GROUP_AT = (3.5, 6.5, 10.5, 15.5, 19.0, 21.5)
HOP = 3.5
DYS = (0, 1, -1, 2)


def kernel(a_ref, m_hbm, mask_ref, out_ref, held, m_ref, part, q_out, s_out, q_in, s_in, total, yq_out, ys_out, yq_in, ys_in,
           m_sem, own_sem, ag_send, ag_recv, z_send, z_recv, zs_send, zs_recv, y_sem):
    row, col = lax.axis_index("row"), lax.axis_index("col")
    core = lax.rem(row, 2)
    x = lax.rem(row // 2, 4)
    y = row // 8
    z = lax.rem(col, 8)
    y_lo = col // 8
    depth = a_ref.shape[0]
    half = depth // 2
    rows = 2 * depth

    def at_xy(dx, dy):
        return ((lax.rem(y + dy + 4, 4) * 4 + lax.rem(x + dx + 4, 4)) * 2 + core, col)

    def at_z(dz):
        return (row, y_lo * 8 + lax.rem(z + dz + 8, 8))

    sibling = ((y * 4 + x) * 2 + (1 - core), col)
    mate = (row, (1 - y_lo) * 8 + z)
    partners = (at_xy(1, 0), at_xy(-1, 0), at_xy(0, 1), at_xy(0, -1), sibling, at_z(1), at_z(-1), mate)

    chunks = m_sem.shape[0]
    step = m_ref.shape[0] // chunks
    loads = [
        pltpu.make_async_copy(m_hbm.at[pl.ds(i * step, step)], m_ref.at[pl.ds(i * step, step)], m_sem.at[i])
        for i in range(chunks)
    ]
    for load in loads:
        load.start()
    own = pltpu.make_async_copy(a_ref, held.at[pl.ds(core * depth, depth)], own_sem)
    own.start()

    barrier = pltpu.get_barrier_semaphore()
    for partner in partners:
        pl.semaphore_signal(barrier, inc=1, device_id=partner, device_id_type=MESH)
    pl.semaphore_wait(barrier, len(partners))

    kinds = {}

    def piece(unit, part_of):
        start = SLOT[unit] * rows + core * depth
        if part_of is None:
            return held.at[pl.ds(start, depth)]
        return held.at[pl.ds(start + part_of * half, half)]

    def message(kind, source, target_unit, part_of, device):
        index = kinds.setdefault(kind, len(kinds))
        return pltpu.make_async_remote_copy(
            src_ref=source, dst_ref=piece(target_unit, part_of), send_sem=ag_send.at[index], recv_sem=ag_recv.at[index],
            device_id=device, device_id_type=MESH)

    sent = {}

    def send(kind, source, target_unit, part_of, device):
        copy = message(kind, source, target_unit, part_of, device)
        copy.start()
        sent[kind] = copy

    def own_half(h):
        return a_ref.at[pl.ds(h * half, half)]

    def source(unit, h):
        if unit == (0, 0):
            return a_ref if h is None else own_half(h)
        return piece(unit, h)

    def wrap(d):
        return 2 if d == -2 else d

    def got(kind):
        sent[kind].wait_recv()

    def to_sibling(unit, h=None):
        send(("s", unit, h), source(unit, h), unit, h, sibling)

    def x_first(dy, h):
        order = (1, -1) if h == 0 else (-1, 1)
        for dx in order:
            send(("x1", dx, dy, h), source((0, dy), h), (-dx, dy), h, at_xy(dx, 0))

    def x_second(dx, dy):
        h = 0 if dx == 1 else 1
        send(("x2", dx, dy), piece((-dx, dy), h), (2, dy), h, at_xy(dx, 0))

    def y_second(dy):
        h = 0 if dy == 1 else 1
        send(("y2", dy), piece((0, -dy), h), (0, 2), h, at_xy(0, dy))

    def act_y1(dy, h):
        def run():
            got(("y1", dy, h))
            first = 0 if dy == 1 else 1
            if h == first:
                y_second(dy)
            x_first(-dy, h)
            if h != first:
                to_sibling((0, -dy))
        return run

    def act_y2(dy):
        def run():
            got(("y2", dy))
            h = 0 if dy == 1 else 1
            x_first(2, h)
            to_sibling((0, 2), h)
        return run

    def act_x1(dx, dy, h):
        def run():
            got(("x1", dx, dy, h))
            if h == (0 if dx == 1 else 1):
                x_second(dx, dy)
            to_sibling((-dx, dy), h)
        return run

    def act_x2(dx, dy):
        def run():
            got(("x2", dx, dy))
            to_sibling((2, dy), 0 if dx == 1 else 1)
        return run

    for h in (0, 1):
        for dy in (1, -1):
            ph = h if dy == 1 else 1 - h
            send(("y1", dy, ph), own_half(ph), (0, -dy), ph, at_xy(0, dy))
        for dx in (1, -1):
            ph = h if dx == 1 else 1 - h
            send(("x1", dx, 0, ph), own_half(ph), (-dx, 0), ph, at_xy(dx, 0))
        if h == 0:
            to_sibling((0, 0))

    tiles = 128
    for i in range(chunks):
        loads[i].wait()

        @pl.loop(0, step // tiles)
        def _(t, i=i):
            for j in range(m_ref.shape[1] // tiles):
                filled = mask_ref[i * (step // tiles) + t, j].astype(jnp.float32)
                here = (pl.ds(pl.multiple_of(i * step + t * tiles, tiles), tiles), pl.ds(j * tiles, tiles))
                m_ref[here] = m_ref[here] * filled.astype(jnp.bfloat16)

    own.wait()

    wide = 256

    def act_mm(lo, hi):
        def run():
            for slot in range(lo, hi):
                for kind in sibling_kinds[slot]:
                    got(kind)
            span = pl.ds(lo * rows, (hi - lo) * rows)

            @pl.loop(0, m_ref.shape[1] // wide)
            def _(n):
                across = pl.ds(pl.multiple_of(n * wide, wide), wide)
                part[span, across] = jnp.dot(held[span, :], m_ref[:, across], preferred_element_type=jnp.float32)
        return run

    lanes = 256

    def encode(value, q_ref, s_ref, t):
        top = jnp.max(jnp.abs(value), axis=0, keepdims=True)
        top = jnp.maximum(top, TINY)
        q_ref[t] = jnp.round(value * (TOP / top)).astype(jnp.int16)
        s_ref[t] = top * (1.0 / TOP)

    def decode(q_ref, s_ref, t):
        return q_ref[t].astype(jnp.float32) * s_ref[t]

    def over_lanes(body):
        pl.loop(0, part.shape[1] // lanes)(body)

    def where_is(slot):
        dx, dy = UNITS[slot]
        ux, uy = lax.rem(x + dx + 4, 4), lax.rem(y + dy + 4, 4)
        lo = uy // 2
        d = lax.rem(z - (lax.rem(uy, 2) * 4 + ux) + 8, 8)
        down = (d < 4) | ((d == 4) & (lo == 0))
        p = jnp.where(d <= 4, d, 8 - d)
        first = (p == 4) | ((p == 3) & (down != (lo == 0)))
        return d, p, down, first, lo

    def z_copies(slot, way, t):
        device = at_z(-1 if way == 0 else 1)
        return (
            pltpu.make_async_remote_copy(
                src_ref=q_out.at[slot, t], dst_ref=q_in.at[slot, way, t],
                send_sem=z_send.at[slot, t], recv_sem=z_recv.at[slot, way, t],
                device_id=device, device_id_type=MESH),
            pltpu.make_async_remote_copy(
                src_ref=s_out.at[slot, t], dst_ref=s_in.at[slot, way, t],
                send_sem=zs_send.at[slot, t], recv_sem=zs_recv.at[slot, way, t],
                device_id=device, device_id_type=MESH),
        )

    def own_part(slot, t):
        return part[pl.ds(slot * rows, rows), pl.ds(pl.multiple_of(t * lanes, lanes), lanes)]

    def act_start(slot):
        def run():
            d, p, down, first, lo = where_is(slot)
            for way in (0, 1):
                @pl.when(first & (down if way == 0 else jnp.logical_not(down)))
                def _():
                    def go(t):
                        encode(own_part(slot, t), q_out.at[slot], s_out.at[slot], t)
                        for copy in z_copies(slot, way, t):
                            copy.start()
                    over_lanes(go)
        return run

    def act_hop(slot, at):
        def run():
            d, p, down, first, lo = where_is(slot)
            for way in (0, 1):
                @pl.when((p == at) & jnp.logical_not(first) & (down if way == 0 else jnp.logical_not(down)))
                def _():
                    def go(t):
                        for copy in z_copies(slot, way, t):
                            copy.wait_recv()
                        encode(own_part(slot, t) + decode(q_in.at[slot, way], s_in.at[slot, way], t),
                               q_out.at[slot], s_out.at[slot], t)
                        for copy in z_copies(slot, way, t):
                            copy.start()
                    over_lanes(go)
        return run

    def y_copies(t):
        return (
            pltpu.make_async_remote_copy(
                src_ref=yq_out.at[t], dst_ref=yq_in.at[t], send_sem=y_sem.at[0, t], recv_sem=y_sem.at[1, t],
                device_id=mate, device_id_type=MESH),
            pltpu.make_async_remote_copy(
                src_ref=ys_out.at[t], dst_ref=ys_in.at[t], send_sem=y_sem.at[2, t], recv_sem=y_sem.at[3, t],
                device_id=mate, device_id_type=MESH),
        )

    def act_end(slot):
        def run():
            d, p, down, first, lo = where_is(slot)

            def summed(t):
                for way in (0, 1):
                    for copy in z_copies(slot, way, t):
                        copy.wait_recv()
                return (own_part(slot, t) + decode(q_in.at[slot, 0], s_in.at[slot, 0], t)
                        + decode(q_in.at[slot, 1], s_in.at[slot, 1], t))

            @pl.when((d == 0) & (lo != y_lo))
            def _():
                def go(t):
                    encode(summed(t), yq_out, ys_out, t)
                    for copy in y_copies(t):
                        copy.start()
                over_lanes(go)

            @pl.when((d == 0) & (lo == y_lo))
            def _():
                def keep(t):
                    total[:, pl.ds(pl.multiple_of(t * lanes, lanes), lanes)] = summed(t)
                over_lanes(keep)
        return run

    acts = []
    for dx in (1, -1):
        f = 0 if dx == 1 else 1
        acts.append((3.0, act_x1(dx, 0, f)))
        acts.append((4.5, act_x1(dx, 0, 1 - f)))
        acts.append((6.3, act_x2(dx, 0)))
        for dy in (1, -1):
            acts.append((9.0, act_x1(dx, dy, f)))
            acts.append((12.0, act_x1(dx, dy, 1 - f)))
            acts.append((13.5, act_x2(dx, dy)))
        acts.append((14.8, act_x1(dx, 2, f)))
        acts.append((16.0, act_x1(dx, 2, 1 - f)))
        acts.append((18.5, act_x2(dx, 2)))
    for dy in (1, -1):
        f = 0 if dy == 1 else 1
        acts.append((5.3, act_y1(dy, f)))
        acts.append((8.1, act_y1(dy, 1 - f)))
        acts.append((11.3, act_y2(dy)))
    for (lo, hi), at in zip(GROUPS, GROUP_AT):
        acts.append((at, act_mm(lo, hi)))
        for slot in range(lo, hi):
            acts.append((at + 0.01, act_start(slot)))
            for k in (3, 2, 1):
                acts.append((at + 1.0 + HOP * (4 - k), act_hop(slot, k)))
            acts.append((at + 1.0 + HOP * 4, act_end(slot)))
    acts.sort(key=lambda act: act[0])

    sibling_kinds = []
    for unit in UNITS:
        dx, dy = unit
        whole = dx == 0 and dy != 2
        sibling_kinds.append([("s", unit, None)] if whole else [("s", unit, 0), ("s", unit, 1)])

    for _, run in acts:
        run()

    def finish(t):
        for copy in y_copies(t):
            copy.wait_recv()
        across = pl.ds(pl.multiple_of(t * lanes, lanes), lanes)
        out_ref[:, across] = total[:, across] + decode(yq_in, ys_in, t)
    over_lanes(finish)

    for copy in sent.values():
        copy.wait_send()
    for slot in range(len(UNITS)):
        d = where_is(slot)[0]

        @pl.when(d != 0)
        def _():
            def gone(t):
                for copy in z_copies(slot, 0, t):
                    copy.wait_send()
            over_lanes(gone)

    def handed(t):
        for copy in y_copies(t):
            copy.wait_send()
    over_lanes(handed)


def gathered_product(amplitudes, integrals, tile_mask):
    depth, inner = amplitudes.shape
    width = integrals.shape[1]
    rows = 2 * depth
    n = len(UNITS)
    groups = width // 256
    vmem = pltpu.VMEM
    dma = pltpu.SemaphoreType.DMA
    messages = 64
    return pl.pallas_call(
        kernel,
        out_shape=jax.ShapeDtypeStruct((rows, width), jnp.float32),
        in_specs=[
            pl.BlockSpec(memory_space=pltpu.HBM),
            pl.BlockSpec(memory_space=pltpu.HBM),
            pl.BlockSpec(memory_space=pltpu.SMEM),
        ],
        out_specs=pl.BlockSpec(memory_space=pltpu.VMEM),
        scratch_shapes=[
            vmem((n * rows, inner), jnp.bfloat16),
            vmem((inner, width), jnp.bfloat16),
            vmem((n * rows, width), jnp.float32),
            vmem((n, groups, rows, 256), jnp.int16),
            vmem((n, groups, 1, 256), jnp.float32),
            vmem((n, 2, groups, rows, 256), jnp.int16),
            vmem((n, 2, groups, 1, 256), jnp.float32),
            vmem((rows, width), jnp.float32),
            vmem((groups, rows, 256), jnp.int16),
            vmem((groups, 1, 256), jnp.float32),
            vmem((groups, rows, 256), jnp.int16),
            vmem((groups, 1, 256), jnp.float32),
            dma((4,)),
            dma,
            dma((messages,)),
            dma((messages,)),
            dma((n, groups)),
            dma((n, 2, groups)),
            dma((n, groups)),
            dma((n, 2, groups)),
            dma((4, groups)),
        ],
        compiler_params=pltpu.CompilerParams(
            collective_id=0, has_side_effects=True, vmem_limit_bytes=63 * 1024 * 1024),
        name="ladder",
    )(amplitudes, integrals, tile_mask)


def shards(amplitudes, integrals, tile_mask, driving, occupied_energy, virtual_energy):
    ladder = gathered_product(amplitudes, integrals, tile_mask)
    denom = virtual_energy[None, :] - occupied_energy[:, None]
    return (driving.astype(jnp.float32) + ladder) / denom


def solution(mesh):
    in_specs = (
        P("row", "col"),
        P("col", "row"),
        P("col", "row"),
        P("col", "row"),
        P("col"),
        P("row"),
    )
    out_specs = P("col", "row")
    return jax.shard_map(shards, mesh=mesh, in_specs=in_specs, out_specs=out_specs, check_vma=False)
```

```python
import functools

import jax
import jax.numpy as jnp
from jax import lax
from jax.experimental import pallas as pl
from jax.experimental.pallas import tpu as pltpu
from jax.sharding import PartitionSpec as P

MESH = pl.DeviceIdType.MESH
TOP = 32767.0
TINY = 1e-30

UNITS = (
    (0, 0),
    (1, 0), (-1, 0),
    (2, 0), (0, 1), (0, -1),
    (1, 1), (1, -1), (-1, 1), (-1, -1), (0, 2),
    (2, 1), (2, -1), (1, 2), (-1, 2),
    (2, 2),
)
SLOT = {unit: slot for slot, unit in enumerate(UNITS)}
GROUPS = ((0, 1), (1, 3), (3, 6), (6, 11), (11, 15), (15, 16))
GROUP_AT = (3.5, 6.5, 10.5, 15.5, 19.0, 21.5)
HOP = 20.0
DYS = (0, 1, -1, 2)


def kernel(a_ref, m_hbm, mask_ref, out_ref, held, m_ref, part, q_out, s_out, q_in, s_in, total, yq_out, ys_out, yq_in, ys_in,
           m_sem, own_sem, ag_send, ag_recv, z_send, z_recv, zs_send, zs_recv, y_sem):
    row, col = lax.axis_index("row"), lax.axis_index("col")
    core = lax.rem(row, 2)
    x = lax.rem(row // 2, 4)
    y = row // 8
    z = lax.rem(col, 8)
    y_lo = col // 8
    depth = a_ref.shape[0]
    half = depth // 2
    rows = 2 * depth

    def at_xy(dx, dy):
        return ((lax.rem(y + dy + 4, 4) * 4 + lax.rem(x + dx + 4, 4)) * 2 + core, col)

    def at_z(dz):
        return (row, y_lo * 8 + lax.rem(z + dz + 8, 8))

    sibling = ((y * 4 + x) * 2 + (1 - core), col)
    mate = (row, (1 - y_lo) * 8 + z)
    partners = (at_xy(1, 0), at_xy(-1, 0), at_xy(0, 1), at_xy(0, -1), sibling, at_z(1), at_z(-1), mate)

    chunks = m_sem.shape[0]
    step = m_ref.shape[0] // chunks
    loads = [
        pltpu.make_async_copy(m_hbm.at[pl.ds(i * step, step)], m_ref.at[pl.ds(i * step, step)], m_sem.at[i])
        for i in range(chunks)
    ]
    for load in loads:
        load.start()
    own = pltpu.make_async_copy(a_ref, held.at[pl.ds(core * depth, depth)], own_sem)
    own.start()

    barrier = pltpu.get_barrier_semaphore()
    for partner in partners:
        pl.semaphore_signal(barrier, inc=1, device_id=partner, device_id_type=MESH)
    pl.semaphore_wait(barrier, len(partners))

    kinds = {}

    def piece(unit, part_of):
        start = SLOT[unit] * rows + core * depth
        if part_of is None:
            return held.at[pl.ds(start, depth)]
        return held.at[pl.ds(start + part_of * half, half)]

    def message(kind, source, target_unit, part_of, device):
        index = kinds.setdefault(kind, len(kinds))
        return pltpu.make_async_remote_copy(
            src_ref=source, dst_ref=piece(target_unit, part_of), send_sem=ag_send.at[index], recv_sem=ag_recv.at[index],
            device_id=device, device_id_type=MESH)

    sent = {}

    def send(kind, source, target_unit, part_of, device):
        copy = message(kind, source, target_unit, part_of, device)
        copy.start()
        sent[kind] = copy

    def own_half(h):
        return a_ref.at[pl.ds(h * half, half)]

    def source(unit, h):
        if unit == (0, 0):
            return a_ref if h is None else own_half(h)
        return piece(unit, h)

    def wrap(d):
        return 2 if d == -2 else d

    def got(kind):
        sent[kind].wait_recv()

    def to_sibling(unit, h=None):
        send(("s", unit, h), source(unit, h), unit, h, sibling)

    def x_first(dy, h):
        order = (1, -1) if h == 0 else (-1, 1)
        for dx in order:
            send(("x1", dx, dy, h), source((0, dy), h), (-dx, dy), h, at_xy(dx, 0))

    def x_second(dx, dy):
        h = 0 if dx == 1 else 1
        send(("x2", dx, dy), piece((-dx, dy), h), (2, dy), h, at_xy(dx, 0))

    def y_second(dy):
        h = 0 if dy == 1 else 1
        send(("y2", dy), piece((0, -dy), h), (0, 2), h, at_xy(0, dy))

    def act_y1(dy, h):
        def run():
            got(("y1", dy, h))
            first = 0 if dy == 1 else 1
            if h == first:
                y_second(dy)
            x_first(-dy, h)
            if h != first:
                to_sibling((0, -dy))
        return run

    def act_y2(dy):
        def run():
            got(("y2", dy))
            h = 0 if dy == 1 else 1
            x_first(2, h)
            to_sibling((0, 2), h)
        return run

    def act_x1(dx, dy, h):
        def run():
            got(("x1", dx, dy, h))
            if h == (0 if dx == 1 else 1):
                x_second(dx, dy)
            to_sibling((-dx, dy), h)
        return run

    def act_x2(dx, dy):
        def run():
            got(("x2", dx, dy))
            to_sibling((2, dy), 0 if dx == 1 else 1)
        return run

    for h in (0, 1):
        for dy in (1, -1):
            ph = h if dy == 1 else 1 - h
            send(("y1", dy, ph), own_half(ph), (0, -dy), ph, at_xy(0, dy))
        for dx in (1, -1):
            ph = h if dx == 1 else 1 - h
            send(("x1", dx, 0, ph), own_half(ph), (-dx, 0), ph, at_xy(dx, 0))
        if h == 0:
            to_sibling((0, 0))

    tiles = 128
    for i in range(chunks):
        loads[i].wait()

        @pl.loop(0, step // tiles)
        def _(t, i=i):
            for j in range(m_ref.shape[1] // tiles):
                filled = mask_ref[i * (step // tiles) + t, j].astype(jnp.float32)
                here = (pl.ds(pl.multiple_of(i * step + t * tiles, tiles), tiles), pl.ds(j * tiles, tiles))
                m_ref[here] = m_ref[here] * filled.astype(jnp.bfloat16)

    own.wait()

    wide = 256

    def act_mm(lo, hi):
        def run():
            for slot in range(lo, hi):
                for kind in sibling_kinds[slot]:
                    got(kind)
            span = pl.ds(lo * rows, (hi - lo) * rows)

            @pl.loop(0, m_ref.shape[1] // wide)
            def _(n):
                across = pl.ds(pl.multiple_of(n * wide, wide), wide)
                part[span, across] = jnp.dot(held[span, :], m_ref[:, across], preferred_element_type=jnp.float32)
        return run

    lanes = 256

    def encode(value, q_ref, s_ref, t):
        top = jnp.max(jnp.abs(value), axis=0, keepdims=True)
        top = jnp.maximum(top, TINY)
        q_ref[t] = jnp.round(value * (TOP / top)).astype(jnp.int16)
        s_ref[t] = top * (1.0 / TOP)

    def decode(q_ref, s_ref, t):
        return q_ref[t].astype(jnp.float32) * s_ref[t]

    def over_lanes(body):
        pl.loop(0, part.shape[1] // lanes)(body)

    def where_is(slot):
        dx, dy = UNITS[slot]
        ux, uy = lax.rem(x + dx + 4, 4), lax.rem(y + dy + 4, 4)
        lo = uy // 2
        d = lax.rem(z - (lax.rem(uy, 2) * 4 + ux) + 8, 8)
        down = (d < 4) | ((d == 4) & (lo == 0))
        p = jnp.where(d <= 4, d, 8 - d)
        first = (p == 4) | ((p == 3) & (down != (lo == 0)))
        return d, p, down, first, lo

    def z_copies(slot, way, t):
        device = at_z(-1 if way == 0 else 1)
        return (
            pltpu.make_async_remote_copy(
                src_ref=q_out.at[slot, t], dst_ref=q_in.at[slot, way, t],
                send_sem=z_send.at[slot, t], recv_sem=z_recv.at[slot, way, t],
                device_id=device, device_id_type=MESH),
            pltpu.make_async_remote_copy(
                src_ref=s_out.at[slot, t], dst_ref=s_in.at[slot, way, t],
                send_sem=zs_send.at[slot, t], recv_sem=zs_recv.at[slot, way, t],
                device_id=device, device_id_type=MESH),
        )

    def own_part(slot, t):
        return part[pl.ds(slot * rows, rows), pl.ds(pl.multiple_of(t * lanes, lanes), lanes)]

    def act_start(slot):
        def run():
            d, p, down, first, lo = where_is(slot)
            for way in (0, 1):
                @pl.when(first & (down if way == 0 else jnp.logical_not(down)))
                def _():
                    def go(t):
                        encode(own_part(slot, t), q_out.at[slot], s_out.at[slot], t)
                        for copy in z_copies(slot, way, t):
                            copy.start()
                    over_lanes(go)
        return run

    def act_hop(slot, at):
        def run():
            d, p, down, first, lo = where_is(slot)
            for way in (0, 1):
                @pl.when((p == at) & jnp.logical_not(first) & (down if way == 0 else jnp.logical_not(down)))
                def _():
                    def go(t):
                        for copy in z_copies(slot, way, t):
                            copy.wait_recv()
                        encode(own_part(slot, t) + decode(q_in.at[slot, way], s_in.at[slot, way], t),
                               q_out.at[slot], s_out.at[slot], t)
                        for copy in z_copies(slot, way, t):
                            copy.start()
                    over_lanes(go)
        return run

    def y_copies(t):
        return (
            pltpu.make_async_remote_copy(
                src_ref=yq_out.at[t], dst_ref=yq_in.at[t], send_sem=y_sem.at[0, t], recv_sem=y_sem.at[1, t],
                device_id=mate, device_id_type=MESH),
            pltpu.make_async_remote_copy(
                src_ref=ys_out.at[t], dst_ref=ys_in.at[t], send_sem=y_sem.at[2, t], recv_sem=y_sem.at[3, t],
                device_id=mate, device_id_type=MESH),
        )

    def act_end(slot):
        def run():
            d, p, down, first, lo = where_is(slot)

            def summed(t):
                for way in (0, 1):
                    for copy in z_copies(slot, way, t):
                        copy.wait_recv()
                return (own_part(slot, t) + decode(q_in.at[slot, 0], s_in.at[slot, 0], t)
                        + decode(q_in.at[slot, 1], s_in.at[slot, 1], t))

            @pl.when((d == 0) & (lo != y_lo))
            def _():
                def go(t):
                    encode(summed(t), yq_out, ys_out, t)
                    for copy in y_copies(t):
                        copy.start()
                over_lanes(go)

            @pl.when((d == 0) & (lo == y_lo))
            def _():
                def keep(t):
                    total[:, pl.ds(pl.multiple_of(t * lanes, lanes), lanes)] = summed(t)
                over_lanes(keep)
        return run

    acts = []
    for dx in (1, -1):
        f = 0 if dx == 1 else 1
        acts.append((3.0, act_x1(dx, 0, f)))
        acts.append((4.5, act_x1(dx, 0, 1 - f)))
        acts.append((6.3, act_x2(dx, 0)))
        for dy in (1, -1):
            acts.append((9.0, act_x1(dx, dy, f)))
            acts.append((12.0, act_x1(dx, dy, 1 - f)))
            acts.append((13.5, act_x2(dx, dy)))
        acts.append((14.8, act_x1(dx, 2, f)))
        acts.append((16.0, act_x1(dx, 2, 1 - f)))
        acts.append((18.5, act_x2(dx, 2)))
    for dy in (1, -1):
        f = 0 if dy == 1 else 1
        acts.append((5.3, act_y1(dy, f)))
        acts.append((8.1, act_y1(dy, 1 - f)))
        acts.append((11.3, act_y2(dy)))
    for (lo, hi), at in zip(GROUPS, GROUP_AT):
        acts.append((at, act_mm(lo, hi)))
        for slot in range(lo, hi):
            acts.append((at + 0.01, act_start(slot)))
            for k in (3, 2, 1):
                acts.append((at + 1.0 + HOP * (4 - k), act_hop(slot, k)))
            acts.append((at + 1.0 + HOP * 4, act_end(slot)))
    acts.sort(key=lambda act: act[0])

    sibling_kinds = []
    for unit in UNITS:
        dx, dy = unit
        whole = dx == 0 and dy != 2
        sibling_kinds.append([("s", unit, None)] if whole else [("s", unit, 0), ("s", unit, 1)])

    for _, run in acts:
        run()

    def finish(t):
        for copy in y_copies(t):
            copy.wait_recv()
        across = pl.ds(pl.multiple_of(t * lanes, lanes), lanes)
        out_ref[:, across] = total[:, across] + decode(yq_in, ys_in, t)
    over_lanes(finish)

    for copy in sent.values():
        copy.wait_send()
    for slot in range(len(UNITS)):
        d = where_is(slot)[0]

        @pl.when(d != 0)
        def _():
            def gone(t):
                for copy in z_copies(slot, 0, t):
                    copy.wait_send()
            over_lanes(gone)

    def handed(t):
        for copy in y_copies(t):
            copy.wait_send()
    over_lanes(handed)


def gathered_product(amplitudes, integrals, tile_mask):
    depth, inner = amplitudes.shape
    width = integrals.shape[1]
    rows = 2 * depth
    n = len(UNITS)
    groups = width // 256
    vmem = pltpu.VMEM
    dma = pltpu.SemaphoreType.DMA
    messages = 64
    return pl.pallas_call(
        kernel,
        out_shape=jax.ShapeDtypeStruct((rows, width), jnp.float32),
        in_specs=[
            pl.BlockSpec(memory_space=pltpu.HBM),
            pl.BlockSpec(memory_space=pltpu.HBM),
            pl.BlockSpec(memory_space=pltpu.SMEM),
        ],
        out_specs=pl.BlockSpec(memory_space=pltpu.VMEM),
        scratch_shapes=[
            vmem((n * rows, inner), jnp.bfloat16),
            vmem((inner, width), jnp.bfloat16),
            vmem((n * rows, width), jnp.float32),
            vmem((n, groups, rows, 256), jnp.int16),
            vmem((n, groups, 1, 256), jnp.float32),
            vmem((n, 2, groups, rows, 256), jnp.int16),
            vmem((n, 2, groups, 1, 256), jnp.float32),
            vmem((rows, width), jnp.float32),
            vmem((groups, rows, 256), jnp.int16),
            vmem((groups, 1, 256), jnp.float32),
            vmem((groups, rows, 256), jnp.int16),
            vmem((groups, 1, 256), jnp.float32),
            dma((4,)),
            dma,
            dma((messages,)),
            dma((messages,)),
            dma((n, groups)),
            dma((n, 2, groups)),
            dma((n, groups)),
            dma((n, 2, groups)),
            dma((4, groups)),
        ],
        compiler_params=pltpu.CompilerParams(
            collective_id=0, has_side_effects=True, vmem_limit_bytes=63 * 1024 * 1024),
        name="ladder",
    )(amplitudes, integrals, tile_mask)


def shards(amplitudes, integrals, tile_mask, driving, occupied_energy, virtual_energy):
    ladder = gathered_product(amplitudes, integrals, tile_mask)
    denom = virtual_energy[None, :] - occupied_energy[:, None]
    return (driving.astype(jnp.float32) + ladder) / denom


def solution(mesh):
    in_specs = (
        P("row", "col"),
        P("col", "row"),
        P("col", "row"),
        P("col", "row"),
        P("col"),
        P("row"),
    )
    out_specs = P("col", "row")
    return jax.shard_map(shards, mesh=mesh, in_specs=in_specs, out_specs=out_specs, check_vma=False)
```

```python
import functools

import jax
import jax.numpy as jnp
from jax import lax
from jax.experimental import pallas as pl
from jax.experimental.pallas import tpu as pltpu
from jax.sharding import PartitionSpec as P

MESH = pl.DeviceIdType.MESH
TOP = 32767.0
TINY = 1e-30

UNITS = (
    (0, 0),
    (1, 0), (-1, 0),
    (2, 0), (0, 1), (0, -1),
    (1, 1), (1, -1), (-1, 1), (-1, -1), (0, 2),
    (2, 1), (2, -1), (1, 2), (-1, 2),
    (2, 2),
)
SLOT = {unit: slot for slot, unit in enumerate(UNITS)}
GROUPS = ((0, 1), (1, 3), (3, 6), (6, 11), (11, 15), (15, 16))
GROUP_AT = (3.5, 6.5, 10.5, 15.5, 19.0, 21.5)
HOP = 20.0
DYS = (0, 1, -1, 2)


def kernel(a_ref, m_hbm, mask_ref, out_ref, held, m_ref, part, q_out, s_out, q_in, s_in, total, yq_out, ys_out, yq_in, ys_in,
           m_sem, own_sem, ag_send, ag_recv, z_send, z_recv, zs_send, zs_recv, y_sem):
    row, col = lax.axis_index("row"), lax.axis_index("col")
    core = lax.rem(row, 2)
    x = lax.rem(row // 2, 4)
    y = row // 8
    z = lax.rem(col, 8)
    y_lo = col // 8
    depth = a_ref.shape[0]
    half = depth // 2
    rows = 2 * depth

    def at_xy(dx, dy):
        return ((lax.rem(y + dy + 4, 4) * 4 + lax.rem(x + dx + 4, 4)) * 2 + core, col)

    def at_z(dz):
        return (row, y_lo * 8 + lax.rem(z + dz + 8, 8))

    sibling = ((y * 4 + x) * 2 + (1 - core), col)
    mate = (row, (1 - y_lo) * 8 + z)
    partners = (at_xy(1, 0), at_xy(-1, 0), at_xy(0, 1), at_xy(0, -1), sibling, at_z(1), at_z(-1), mate)

    chunks = m_sem.shape[0]
    step = m_ref.shape[0] // chunks
    loads = [
        pltpu.make_async_copy(m_hbm.at[pl.ds(i * step, step)], m_ref.at[pl.ds(i * step, step)], m_sem.at[i])
        for i in range(chunks)
    ]
    for load in loads:
        load.start()
    own = pltpu.make_async_copy(a_ref, held.at[pl.ds(core * depth, depth)], own_sem)
    own.start()

    barrier = pltpu.get_barrier_semaphore()
    for partner in partners:
        pl.semaphore_signal(barrier, inc=1, device_id=partner, device_id_type=MESH)
    pl.semaphore_wait(barrier, len(partners))

    kinds = {}

    def piece(unit, part_of):
        start = SLOT[unit] * rows + core * depth
        if part_of is None:
            return held.at[pl.ds(start, depth)]
        return held.at[pl.ds(start + part_of * half, half)]

    def message(kind, source, target_unit, part_of, device):
        index = kinds.setdefault(kind, len(kinds))
        return pltpu.make_async_remote_copy(
            src_ref=source, dst_ref=piece(target_unit, part_of), send_sem=ag_send.at[index], recv_sem=ag_recv.at[index],
            device_id=device, device_id_type=MESH)

    sent = {}

    def send(kind, source, target_unit, part_of, device):
        copy = message(kind, source, target_unit, part_of, device)
        copy.start()
        sent[kind] = copy

    def own_half(h):
        return a_ref.at[pl.ds(h * half, half)]

    def source(unit, h):
        if unit == (0, 0):
            return a_ref if h is None else own_half(h)
        return piece(unit, h)

    def wrap(d):
        return 2 if d == -2 else d

    def got(kind):
        sent[kind].wait_recv()

    def to_sibling(unit, h=None):
        send(("s", unit, h), source(unit, h), unit, h, sibling)

    def x_first(dy, h):
        order = (1, -1) if h == 0 else (-1, 1)
        for dx in order:
            send(("x1", dx, dy, h), source((0, dy), h), (-dx, dy), h, at_xy(dx, 0))

    def x_second(dx, dy):
        h = 0 if dx == 1 else 1
        send(("x2", dx, dy), piece((-dx, dy), h), (2, dy), h, at_xy(dx, 0))

    def y_second(dy):
        h = 0 if dy == 1 else 1
        send(("y2", dy), piece((0, -dy), h), (0, 2), h, at_xy(0, dy))

    def act_y1(dy, h):
        def run():
            got(("y1", dy, h))
            first = 0 if dy == 1 else 1
            if h == first:
                y_second(dy)
            x_first(-dy, h)
            if h != first:
                to_sibling((0, -dy))
        return run

    def act_y2(dy):
        def run():
            got(("y2", dy))
            h = 0 if dy == 1 else 1
            x_first(2, h)
            to_sibling((0, 2), h)
        return run

    def act_x1(dx, dy, h):
        def run():
            got(("x1", dx, dy, h))
            if h == (0 if dx == 1 else 1):
                x_second(dx, dy)
            to_sibling((-dx, dy), h)
        return run

    def act_x2(dx, dy):
        def run():
            got(("x2", dx, dy))
            to_sibling((2, dy), 0 if dx == 1 else 1)
        return run

    for h in (0, 1):
        for dy in (1, -1):
            ph = h if dy == 1 else 1 - h
            send(("y1", dy, ph), own_half(ph), (0, -dy), ph, at_xy(0, dy))
        for dx in (1, -1):
            ph = h if dx == 1 else 1 - h
            send(("x1", dx, 0, ph), own_half(ph), (-dx, 0), ph, at_xy(dx, 0))
        if h == 0:
            to_sibling((0, 0))

    tiles = 128
    for i in range(chunks):
        loads[i].wait()

        @pl.loop(0, step // tiles)
        def _(t, i=i):
            for j in range(m_ref.shape[1] // tiles):
                filled = mask_ref[i * (step // tiles) + t, j].astype(jnp.float32)
                here = (pl.ds(pl.multiple_of(i * step + t * tiles, tiles), tiles), pl.ds(j * tiles, tiles))
                m_ref[here] = m_ref[here] * filled.astype(jnp.bfloat16)

    own.wait()

    wide = 256

    def act_mm(lo, hi):
        def run():
            for slot in range(lo, hi):
                for kind in sibling_kinds[slot]:
                    got(kind)
            span = pl.ds(lo * rows, (hi - lo) * rows)

            @pl.loop(0, m_ref.shape[1] // wide)
            def _(n):
                across = pl.ds(pl.multiple_of(n * wide, wide), wide)
                part[span, across] = jnp.dot(held[span, :], m_ref[:, across], preferred_element_type=jnp.float32)
        return run

    lanes = 256

    def encode(value, q_ref, s_ref, t):
        top = jnp.max(jnp.abs(value), axis=0, keepdims=True)
        top = jnp.maximum(top, TINY)
        q_ref[t] = jnp.round(value * (TOP / top)).astype(jnp.int16)
        s_ref[t] = top * (1.0 / TOP)

    def decode(q_ref, s_ref, t):
        return q_ref[t].astype(jnp.float32) * s_ref[t]

    def over_lanes(body):
        pl.loop(0, part.shape[1] // lanes)(body)

    def where_is(slot):
        dx, dy = UNITS[slot]
        ux, uy = lax.rem(x + dx + 4, 4), lax.rem(y + dy + 4, 4)
        lo = uy // 2
        d = lax.rem(z - (lax.rem(uy, 2) * 4 + ux) + 8, 8)
        down = (d < 4) | ((d == 4) & (lo == 0))
        p = jnp.where(d <= 4, d, 8 - d)
        first = (p == 4) | ((p == 3) & (down != (lo == 0)))
        return d, p, down, first, lo

    def z_copies(slot, way, t):
        device = at_z(-1 if way == 0 else 1)
        return (
            pltpu.make_async_remote_copy(
                src_ref=q_out.at[slot, t], dst_ref=q_in.at[slot, way, t],
                send_sem=z_send.at[slot, t], recv_sem=z_recv.at[slot, way, t],
                device_id=device, device_id_type=MESH),
            pltpu.make_async_remote_copy(
                src_ref=s_out.at[slot, t], dst_ref=s_in.at[slot, way, t],
                send_sem=zs_send.at[slot, t], recv_sem=zs_recv.at[slot, way, t],
                device_id=device, device_id_type=MESH),
        )

    def own_part(slot, t):
        return part[pl.ds(slot * rows, rows), pl.ds(pl.multiple_of(t * lanes, lanes), lanes)]

    def act_start(slot):
        def run():
            d, p, down, first, lo = where_is(slot)
            for way in (0, 1):
                @pl.when(first & (down if way == 0 else jnp.logical_not(down)))
                def _():
                    def go(t):
                        encode(own_part(slot, t), q_out.at[slot], s_out.at[slot], t)
                        for copy in z_copies(slot, way, t):
                            copy.start()
                    over_lanes(go)
        return run

    def act_hop(slot, at):
        def run():
            d, p, down, first, lo = where_is(slot)
            for way in (0, 1):
                @pl.when((p == at) & jnp.logical_not(first) & (down if way == 0 else jnp.logical_not(down)))
                def _():
                    def go(t):
                        for copy in z_copies(slot, way, t):
                            copy.wait_recv()
                        encode(own_part(slot, t) + decode(q_in.at[slot, way], s_in.at[slot, way], t),
                               q_out.at[slot], s_out.at[slot], t)
                        for copy in z_copies(slot, way, t):
                            copy.start()
                    over_lanes(go)
        return run

    def y_copies(t):
        return (
            pltpu.make_async_remote_copy(
                src_ref=yq_out.at[t], dst_ref=yq_in.at[t], send_sem=y_sem.at[0, t], recv_sem=y_sem.at[1, t],
                device_id=mate, device_id_type=MESH),
            pltpu.make_async_remote_copy(
                src_ref=ys_out.at[t], dst_ref=ys_in.at[t], send_sem=y_sem.at[2, t], recv_sem=y_sem.at[3, t],
                device_id=mate, device_id_type=MESH),
        )

    def act_end(slot, give):
        def run():
            d, p, down, first, lo = where_is(slot)

            def summed(t):
                for way in (0, 1):
                    for copy in z_copies(slot, way, t):
                        copy.wait_recv()
                return (own_part(slot, t) + decode(q_in.at[slot, 0], s_in.at[slot, 0], t)
                        + decode(q_in.at[slot, 1], s_in.at[slot, 1], t))

            @pl.when((d == 0) & ((lo != y_lo) if give else (lo == y_lo)))
            def _():
                def go(t):
                    if give:
                        encode(summed(t), yq_out, ys_out, t)
                        for copy in y_copies(t):
                            copy.start()
                    else:
                        total[:, pl.ds(pl.multiple_of(t * lanes, lanes), lanes)] = summed(t)
                over_lanes(go)
        return run

    acts = []
    for dx in (1, -1):
        f = 0 if dx == 1 else 1
        acts.append((3.0, act_x1(dx, 0, f)))
        acts.append((4.5, act_x1(dx, 0, 1 - f)))
        acts.append((6.3, act_x2(dx, 0)))
        for dy in (1, -1):
            acts.append((9.0, act_x1(dx, dy, f)))
            acts.append((12.0, act_x1(dx, dy, 1 - f)))
            acts.append((13.5, act_x2(dx, dy)))
        acts.append((14.8, act_x1(dx, 2, f)))
        acts.append((16.0, act_x1(dx, 2, 1 - f)))
        acts.append((18.5, act_x2(dx, 2)))
    for dy in (1, -1):
        f = 0 if dy == 1 else 1
        acts.append((5.3, act_y1(dy, f)))
        acts.append((8.1, act_y1(dy, 1 - f)))
        acts.append((11.3, act_y2(dy)))
    for (lo, hi), at in zip(GROUPS, GROUP_AT):
        acts.append((at, act_mm(lo, hi)))
        for slot in range(lo, hi):
            acts.append((at + 0.01, act_start(slot)))
            for k in (3, 2, 1):
                acts.append((at + 1.0 + HOP * (4 - k), act_hop(slot, k)))
            acts.append((at + 1.0 + HOP * 4, act_end(slot, True)))
            acts.append((at + 1.0 + HOP * 6, act_end(slot, False)))
    acts.sort(key=lambda act: act[0])

    sibling_kinds = []
    for unit in UNITS:
        dx, dy = unit
        whole = dx == 0 and dy != 2
        sibling_kinds.append([("s", unit, None)] if whole else [("s", unit, 0), ("s", unit, 1)])

    for _, run in acts:
        run()

    def finish(t):
        for copy in y_copies(t):
            copy.wait_recv()
        across = pl.ds(pl.multiple_of(t * lanes, lanes), lanes)
        out_ref[:, across] = total[:, across] + decode(yq_in, ys_in, t)
    over_lanes(finish)

    for copy in sent.values():
        copy.wait_send()
    for slot in range(len(UNITS)):
        d = where_is(slot)[0]

        @pl.when(d != 0)
        def _():
            def gone(t):
                for copy in z_copies(slot, 0, t):
                    copy.wait_send()
            over_lanes(gone)

    def handed(t):
        for copy in y_copies(t):
            copy.wait_send()
    over_lanes(handed)


def gathered_product(amplitudes, integrals, tile_mask):
    depth, inner = amplitudes.shape
    width = integrals.shape[1]
    rows = 2 * depth
    n = len(UNITS)
    groups = width // 256
    vmem = pltpu.VMEM
    dma = pltpu.SemaphoreType.DMA
    messages = 64
    return pl.pallas_call(
        kernel,
        out_shape=jax.ShapeDtypeStruct((rows, width), jnp.float32),
        in_specs=[
            pl.BlockSpec(memory_space=pltpu.HBM),
            pl.BlockSpec(memory_space=pltpu.HBM),
            pl.BlockSpec(memory_space=pltpu.SMEM),
        ],
        out_specs=pl.BlockSpec(memory_space=pltpu.VMEM),
        scratch_shapes=[
            vmem((n * rows, inner), jnp.bfloat16),
            vmem((inner, width), jnp.bfloat16),
            vmem((n * rows, width), jnp.float32),
            vmem((n, groups, rows, 256), jnp.int16),
            vmem((n, groups, 1, 256), jnp.float32),
            vmem((n, 2, groups, rows, 256), jnp.int16),
            vmem((n, 2, groups, 1, 256), jnp.float32),
            vmem((rows, width), jnp.float32),
            vmem((groups, rows, 256), jnp.int16),
            vmem((groups, 1, 256), jnp.float32),
            vmem((groups, rows, 256), jnp.int16),
            vmem((groups, 1, 256), jnp.float32),
            dma((4,)),
            dma,
            dma((messages,)),
            dma((messages,)),
            dma((n, groups)),
            dma((n, 2, groups)),
            dma((n, groups)),
            dma((n, 2, groups)),
            dma((4, groups)),
        ],
        compiler_params=pltpu.CompilerParams(
            collective_id=0, has_side_effects=True, vmem_limit_bytes=63 * 1024 * 1024),
        name="ladder",
    )(amplitudes, integrals, tile_mask)


def shards(amplitudes, integrals, tile_mask, driving, occupied_energy, virtual_energy):
    ladder = gathered_product(amplitudes, integrals, tile_mask)
    denom = virtual_energy[None, :] - occupied_energy[:, None]
    return (driving.astype(jnp.float32) + ladder) / denom


def solution(mesh):
    in_specs = (
        P("row", "col"),
        P("col", "row"),
        P("col", "row"),
        P("col", "row"),
        P("col"),
        P("row"),
    )
    out_specs = P("col", "row")
    return jax.shard_map(shards, mesh=mesh, in_specs=in_specs, out_specs=out_specs, check_vma=False)
```
